32 devices in a mesh: dp: 1 (over z), sp: 32 (over x, y, core).
Axes of the slice: x: 4, y: 4, z: 1, core: 2. Of those that a mesh axis runs over, the one named last changes fastest.
The devices are a block of a 4x4x8 slice.
Arguments:
- x: bfloat16 [4096, 5120], P(('dp', 'sp'))
- gain: bfloat16 [5120], replicated
- wq: bfloat16 [5120, 4096], replicated
- wk: bfloat16 [5120, 1024], replicated
- wv: bfloat16 [5120, 1024], replicated
- wo: bfloat16 [4096, 5120], replicated
Outputs:
- output: bfloat16 [4096, 5120], P(('dp', 'sp'))
All inputs are finite; a program needn't handle non-finite values.
Results may differ from the reference program's by a relative error of at most 0.012.
Values are sent between devices in bfloat16 or wider.
A program may use at most 768 MiB of HBM per device.

```python
import jax
import jax.numpy as jnp
from jax import lax

ROWS = 4096
D = 5120
HEADS = 32
KV_HEADS = 8
HEAD = 128
THETA = 10000


def setup_inputs(seed: int = 0, part: int = 0) -> dict:
    kx, kn, kq, kk, kv, ko = jax.random.split(jax.random.key(seed), 6)

    def weights(key, rows, columns):
        return jax.random.normal(key, (rows, columns), jnp.float32) * rows**-0.5

    drawn = {
        "x": jax.random.normal(jax.random.fold_in(kx, part), (ROWS, D), jnp.float32),
        "gain": 1 + 0.1 * jax.random.normal(kn, (D,), jnp.float32),
        "wq": 2 * weights(kq, D, HEADS * HEAD),
        "wk": 2 * weights(kk, D, KV_HEADS * HEAD),
        "wv": 4 * weights(kv, D, KV_HEADS * HEAD),
        "wo": weights(ko, HEADS * HEAD, D),
    }
    return {k: v.astype(jnp.bfloat16) for k, v in drawn.items()}


def normed(x, gain):
    wide = x.astype(jnp.float32)
    scale = lax.rsqrt(jnp.mean(wide * wide, -1, keepdims=True) + 1e-6)
    return (wide * scale * gain.astype(jnp.float32)).astype(jnp.bfloat16)


def turned(t, place, theta):
    half = t.shape[-1] // 2
    angle = place.astype(jnp.float32)[:, None] * theta ** (-jnp.arange(half, dtype=jnp.float32) / half)
    cos, sin = jnp.cos(angle)[:, None], jnp.sin(angle)[:, None]
    a, b = t[..., :half].astype(jnp.float32), t[..., half:].astype(jnp.float32)
    return jnp.concatenate([a * cos - b * sin, b * cos + a * sin], -1).astype(jnp.bfloat16)


def matmul(a, w):
    return jnp.dot(a, w, preferred_element_type=jnp.float32).astype(jnp.bfloat16)


def einsum(form, a, b):
    return jnp.einsum(form, a.astype(jnp.float32), b.astype(jnp.float32))


def attention(q, k, v):
    scores = einsum("tgsd,ugd->gstu", q, k) * q.shape[-1] ** -0.5
    token = jnp.arange(q.shape[0])
    scores = jnp.where(token[:, None] >= token, scores, -jnp.inf)
    weights = jax.nn.softmax(scores, -1).astype(jnp.bfloat16)
    return einsum("gstu,ugd->tgsd", weights, v).astype(jnp.bfloat16)


def reference(x, gain, wq, wk, wv, wo):
    a, place = normed(x, gain), jnp.arange(ROWS)
    q = turned(matmul(a, wq).reshape(ROWS, HEADS, HEAD), place, THETA).reshape(ROWS, KV_HEADS, -1, HEAD)
    k = turned(matmul(a, wk).reshape(ROWS, KV_HEADS, HEAD), place, THETA)
    v = matmul(a, wv).reshape(ROWS, KV_HEADS, HEAD)
    seen = attention(q, k, v).reshape(ROWS, HEADS * HEAD)
    return (x.astype(jnp.float32) + jnp.dot(seen, wo, preferred_element_type=jnp.float32)).astype(jnp.bfloat16)
```

```python
import functools

import jax
import jax.numpy as jnp
from jax import lax
from jax.experimental import pallas as pl
from jax.experimental.pallas import tpu as pltpu
from jax.sharding import PartitionSpec as P

HEAD = 128
THETA = 10000
NEG = -1e30
HIDDEN = 2 * NEG
LOG2E = 1.4426950408889634
WIDE = 256
SLOTS = 16
MESH = pl.DeviceIdType.MESH
F32, BF16 = jnp.float32, jnp.bfloat16


def _dot(a, b, ca, cb):
    return lax.dot_general(a, b, (((ca,), (cb,)), ((), ())), preferred_element_type=F32)


def _kernel(n, kv_heads, x_ref, gain_ref, cos_ref, sin_ref, wq_ref, wk_ref, wv_ref, wo_ref, y_ref,
            xs, a_s, ring, kv_st, q_st, kv_all, q_all, o_st, o_all, acc, s0, s1, p0, p1, m0, m1, keep0, keep1, top, mix,
            wsem, xsem, kvs, kvr, rls, rlr, qs, qr, outs, outr):
    own, d = x_ref.shape
    chips, tokens = n // 2, 2 * own
    slices = d // WIDE
    share = n // kv_heads // 2
    half_kv = kv_heads // 2
    kv_slabs = half_kv * HEAD // WIDE
    q_slabs = chips // 2
    me = lax.axis_index("sp")
    chip, core = lax.div(me, 2), lax.rem(me, 2)
    mate = me + 1 - 2 * core
    scale = HEAD**-0.5
    e = scale * LOG2E

    def remote(src, dst, ssem, rsem, device):
        return pltpu.make_async_remote_copy(src_ref=src, dst_ref=dst, send_sem=ssem, recv_sem=rsem, device_id={"sp": device},
                                            device_id_type=MESH)

    def landed(dst, rsem):
        remote(dst, dst, rsem, rsem, mate).wait_recv()

    def sent(src, ssem):
        remote(src, src, ssem, ssem, mate).wait_send()

    own_x = pltpu.make_async_copy(x_ref, xs.at[core], xsem.at[0])
    own_x.start()
    bar = pltpu.get_barrier_semaphore()

    def greet(k, _):
        pl.semaphore_signal(bar, inc=1, device_id={"sp": lax.rem(me + k, n)}, device_id_type=MESH)

    lax.fori_loop(1, n, greet, None)

    def fetch(w_ref, column, slot):
        pltpu.make_async_copy(w_ref.at[:, :, pl.ds(pl.multiple_of(column, WIDE), WIDE)], ring.at[slot], wsem.at[slot]).start()

    def kv_turn(u):
        return lax.rem(u + chip, kv_slabs)

    for u in range(kv_slabs):
        column = core * half_kv * HEAD + kv_turn(u) * WIDE
        fetch(wk_ref, column, 2 * u)
        fetch(wv_ref, column, 2 * u + 1)
    first_q = 2 * kv_slabs

    def q_target(t):
        return lax.rem(chip + 2 * t + 1 + core, chips)

    def fetch_q(t, _):
        fetch(wq_ref, q_target(t) * WIDE, first_q + t)

    lax.fori_loop(0, q_slabs, fetch_q, None)
    ahead = SLOTS - first_q - q_slabs

    def wo_slot(w):
        return lax.rem(first_q + q_slabs + w, SLOTS)

    def fetch_wo(w):
        rows = pl.ds(pl.multiple_of(lax.rem(chip + 1 + w, chips) * WIDE, WIDE), WIDE)
        slot = wo_slot(w)

        def piece(i, _):
            pltpu.make_async_copy(wo_ref.at[rows, pl.ds(pl.multiple_of(i * WIDE, WIDE), WIDE)], ring.at[slot, i], wsem.at[slot]).start()

        lax.fori_loop(0, slices, piece, None)

    lax.fori_loop(0, ahead, lambda w, _: fetch_wo(w), None)

    def slab_ready(slot):
        pltpu.make_async_copy(ring.at[slot], ring.at[slot], wsem.at[slot]).wait()

    pl.semaphore_wait(bar, n - 1)
    give_x = remote(x_ref, xs.at[core], xsem.at[1], xsem.at[2], mate)
    give_x.start()

    def norm(which):
        def rows16(r, _):
            wide = xs[which, pl.ds(pl.multiple_of(r * 16, 16), 16), :].astype(F32)
            inv = lax.rsqrt(jnp.mean(wide * wide, -1, keepdims=True) + 1e-6)
            at = pl.multiple_of(which * own + r * 16, 16)
            a_s[pl.ds(at, 16), :] = (wide * inv * gain_ref[...].astype(F32)).astype(BF16)

        lax.fori_loop(0, own // 16, rows16, None)

    own_x.wait()
    norm(core)
    acc[...] = xs[core].astype(F32)
    landed(xs.at[1 - core], xsem.at[2])
    norm(1 - core)

    def product(slot):
        slab_ready(slot)
        return jnp.dot(a_s[...], ring[slot].reshape(d, WIDE), preferred_element_type=F32).astype(BF16)

    def turned(t):
        f = t.astype(F32)
        return (f * cos_ref[...] + pltpu.roll(f, HEAD // 2, 1) * sin_ref[...]).astype(BF16)

    for u in range(kv_slabs):
        for kind in range(2):
            slab = 2 * u + kind
            r = product(slab)
            fetch_wo(ahead + slab)
            for b in range(2):
                t = r[:, b * HEAD : (b + 1) * HEAD]
                t = turned(t) if kind == 0 else jnp.concatenate([t[:own].T, t[own:].T], axis=0)
                kv_st[slab, b] = t
                g = core * half_kv + kv_turn(u) * 2 + b
                for i in range(share):
                    device = 2 * (share * g + i) + kind

                    @pl.when(device != me)
                    def _():
                        remote(kv_st.at[slab, b], kv_all.at[kind, chip], kvs.at[slab, b, i], kvr.at[chip], device).start()

                    @pl.when(device == me)
                    def _():
                        kv_all[kind, chip] = t

    def q_turn(t, _):
        slab = first_q + t
        r = product(slab)
        fetch_wo(ahead + slab)
        for b in range(2):
            q = turned(r[:, b * HEAD : (b + 1) * HEAD])
            q_st[t, b] = q
            device = 2 * q_target(t) + b

            @pl.when(device != me)
            def _():
                remote(q_st.at[t, b], q_all.at[chip], qs.at[t, b], qr.at[chip], device).start()

            @pl.when(device == me)
            def _():
                q_all[chip] = q

    lax.fori_loop(0, q_slabs, q_turn, None)

    kv_core = lax.div(lax.div(chip, share), half_kv)

    def pass_on(r, _):
        src = lax.rem(chip + r, chips)

        @pl.when(2 * src + kv_core != me)
        def _():
            landed(kv_all.at[core, src], kvr.at[src])

        remote(kv_all.at[core, src], kv_all.at[core, src], rls.at[src], rlr.at[src], mate).start()

    lax.fori_loop(0, chips, pass_on, None)
    lax.fori_loop(0, chips, lambda r, _: landed(kv_all.at[1 - core, r], rlr.at[r]), None)

    span = 2 * tokens

    def source(t):
        return lax.rem(chip - 1 - t + 2 * chips, chips)

    def last(t):
        return lax.div(source(t), 2)

    for ref in (s0, s1, p0, p1, m0, m1, keep0, keep1, top, mix):
        ref[...] = jnp.zeros_like(ref)

    def stage(par, it, at_a, at_b, at_c):
        (ta, ka), (tb, kb), (tc, kc) = at_a, at_b, at_c
        s_new, s_old = (s0, s1)[par], (s1, s0)[par]
        m_new, m_old = (m0, m1)[par], (m1, m0)[par]
        p_new, p_old = (p0, p1)[par], (p1, p0)[par]
        keep_new, keep_old = (keep0, keep1)[par], (keep1, keep0)[par]
        src = source(ta)
        sender = 2 * src + lax.rem(ta, 2)

        @pl.when((ka == 0) & (ta < chips) & (sender != me))
        def _():
            landed(q_all.at[src], qr.at[src])

        def work(masked):
            v = kv_all[1, pl.ds(2 * kc, 2)]
            v = jnp.concatenate([v[i, j * HEAD : (j + 1) * HEAD] for i in range(2) for j in range(2)], axis=1)
            v = jnp.concatenate([v, jnp.ones((16, span), BF16)], axis=0)
            mix[...] = mix[...] * keep_old[...] + _dot(v, p_old[...], 1, 0)
            s = _dot(kv_all[0, pl.ds(2 * ka, 2)].reshape(span, HEAD), q_all[src], 1, 1)
            if masked:
                gap = lax.broadcasted_iota(jnp.int32, s.shape, 1) - lax.broadcasted_iota(jnp.int32, s.shape, 0)
                s = jnp.where(gap >= span * ka - tokens * src, s, HIDDEN)
            s_new[...] = s
            m_new[...] = s.max(axis=0, keepdims=True)
            before = jnp.where(kb == 0, NEG, top[...])
            after = jnp.maximum(before, m_old[...])
            top[...] = after
            p_new[...] = jnp.exp2((s_old[...] - after) * e).astype(BF16)
            keep_new[...] = jnp.exp2((before - after) * e)

        ragged = ka == last(ta)
        pl.when(ragged)(lambda: work(True))
        pl.when(jnp.logical_not(ragged))(lambda: work(False))

        @pl.when((kc == last(tc)) & (it >= 2))
        def _():
            to = source(tc)
            o = (mix[:HEAD, :] * (1 / mix[HEAD : HEAD + 1, :])).T.astype(BF16)
            o_st[to] = o
            for b in range(2):
                device = 2 * to + b

                @pl.when(device != me)
                def _():
                    remote(o_st.at[to, pl.ds(b * own, own)], o_all.at[me], outs.at[to, b], outr.at[me], device).start()

                @pl.when(device == me)
                def _():
                    o_all[me] = o[b * own : (b + 1) * own]

        step = ka == last(ta)
        return (jnp.where(step, ta + 1, ta), jnp.where(step, 0, ka + 1)), at_a, at_b

    def two(i, at):
        at = stage(0, 2 * i, *at)
        return stage(1, 2 * i + 1, *at)

    pairs = sum(i // 2 + 1 for i in range(chips)) + 2
    zero = (jnp.int32(0), jnp.int32(0))
    lax.fori_loop(0, pairs // 2, two, (zero, zero, zero))

    def back(w, _):
        j = lax.rem(chip + 1 + w, chips)
        for b in range(2):

            @pl.when(2 * j + b != me)
            def _():
                landed(o_all.at[2 * j + b], outr.at[2 * j + b])

        slot = wo_slot(w)
        slab_ready(slot)
        o = jnp.concatenate([o_all[2 * j], o_all[2 * j + 1]], axis=1)
        for i in range(slices):
            acc[:, i * WIDE : (i + 1) * WIDE] += jnp.dot(o, ring[slot, i], preferred_element_type=F32)

    lax.fori_loop(0, chips, back, None)
    y_ref[...] = acc[...].astype(BF16)

    give_x.wait_send()
    for u in range(kv_slabs):
        for kind in range(2):
            for b in range(2):
                for i in range(share):

                    @pl.when(2 * (share * (core * half_kv + kv_turn(u) * 2 + b) + i) + kind != me)
                    def _():
                        sent(kv_st.at[2 * u + kind, b], kvs.at[2 * u + kind, b, i])

    def q_sent(t, _):
        for b in range(2):

            @pl.when(2 * q_target(t) + b != me)
            def _():
                sent(q_st.at[t, b], qs.at[t, b])

    lax.fori_loop(0, q_slabs, q_sent, None)

    def rest_sent(i, _):
        sent(kv_all.at[core, i], rls.at[i])
        for b in range(2):

            @pl.when(2 * i + b != me)
            def _():
                sent(o_st.at[i, pl.ds(b * own, own)], outs.at[i, b])

    lax.fori_loop(0, chips, rest_sent, None)


def solution(mesh):
    n = mesh.shape["sp"]

    def step(x, gain, wq, wk, wv, wo):
        own, d = x.shape
        chips, tokens = n // 2, 2 * own
        kv_heads = wk.shape[1] // HEAD
        half = HEAD // 2
        place = lax.axis_index("sp") // 2 * tokens + jnp.arange(tokens)
        angle = place.astype(F32)[:, None] * THETA ** (-jnp.arange(half, dtype=F32) / half)
        cos, sin = jnp.cos(angle), jnp.sin(angle)
        cos, sin = jnp.concatenate([cos, cos], 1), jnp.concatenate([-sin, sin], 1)
        cut = lambda w: w.reshape(d // WIDE, WIDE, w.shape[1])
        dma = pltpu.SemaphoreType.DMA
        kv_slabs = kv_heads * HEAD // WIDE
        hbm, vmem = pl.BlockSpec(memory_space=pltpu.HBM), pl.BlockSpec(memory_space=pltpu.VMEM)
        span = 2 * tokens
        return pl.pallas_call(
            functools.partial(_kernel, n, kv_heads),
            out_shape=jax.ShapeDtypeStruct((own, d), BF16),
            in_specs=[hbm, vmem, vmem, vmem, hbm, hbm, hbm, hbm],
            out_specs=vmem,
            scratch_shapes=[
                pltpu.VMEM((2, own, d), BF16),
                pltpu.VMEM((tokens, d), BF16),
                pltpu.VMEM((SLOTS, d // WIDE, WIDE, WIDE), BF16),
                pltpu.VMEM((kv_slabs, 2, tokens, HEAD), BF16),
                pltpu.VMEM((chips // 2, 2, tokens, HEAD), BF16),
                pltpu.VMEM((2, chips, tokens, HEAD), BF16),
                pltpu.VMEM((chips, tokens, HEAD), BF16),
                pltpu.VMEM((chips, tokens, HEAD), BF16),
                pltpu.VMEM((n, own, HEAD), BF16),
                pltpu.VMEM((own, d), F32),
                *[pltpu.VMEM((span, tokens), F32)] * 2,
                *[pltpu.VMEM((span, tokens), BF16)] * 2,
                *[pltpu.VMEM((1, tokens), F32)] * 5,
                pltpu.VMEM((HEAD + 16, tokens), F32),
                dma((SLOTS,)), dma((3,)), dma((kv_slabs, 2, n // kv_heads // 2)), dma((chips,)), dma((chips,)), dma((chips,)),
                dma((chips // 2, 2)), dma((chips,)), dma((chips, 2)), dma((n,)),
            ],
            compiler_params=pltpu.CompilerParams(collective_id=0, has_side_effects=True, vmem_limit_bytes=67043328),
        )(x, gain[None], cos, sin, cut(wq), cut(wk), cut(wv), wo)

    tokens, whole = P(("dp", "sp"), None), P(None, None)
    return jax.shard_map(
        step,
        mesh=mesh,
        in_specs=(tokens, P(None), whole, whole, whole, whole),
        out_specs=tokens,
        check_vma=False,
    )
```

```python
import functools

import jax
import jax.numpy as jnp
import numpy as np
from jax import lax
from jax.experimental import pallas as pl
from jax.experimental.pallas import tpu as pltpu
from jax.sharding import PartitionSpec as P

HEAD = 128
THETA = 10000
NEG = -1e30
HIDDEN = 2 * NEG
LOG2E = 1.4426950408889634
WIDE = 256
SLOTS = 5
WO_SLOTS = 10
MESH = pl.DeviceIdType.MESH
F32, BF16 = jnp.float32, jnp.bfloat16


def _dot(a, b, ca, cb):
    return lax.dot_general(a, b, (((ca,), (cb,)), ((), ())), preferred_element_type=F32)


def _kernel(n, kv_heads, x_ref, gain_ref, turn_ref, wq_ref, wk_ref, wv_ref, wo_ref, y_ref,
            cos_ref, sin_ref, xs, ring, wo_ring, kv_st, q_st, kv_all, q_all, o_st, o_all, acc, s0, s1, p0, p1, m0, m1, keep0, keep1, top, mix,
            wsem, wosem, xsem, kvs, kvr, nears, nearr, fars, fark, farv, qs, qr, outs, outr):
    own, d = x_ref.shape
    chips, tokens = n // 2, 2 * own
    slices = d // WIDE
    nx = kv_heads // 2
    ny = chips // nx
    pairs = n // kv_heads // 2
    me = lax.axis_index("sp")
    chip, core = lax.div(me, 2), lax.rem(me, 2)
    x, y = lax.div(chip, ny), lax.rem(chip, ny)
    mate = me + 1 - 2 * core
    scale = HEAD**-0.5
    e = scale * LOG2E

    def at(i, j, k):
        return (i * ny + j) * 2 + k

    def along(i):
        return lax.rem(x + i, nx)

    def remote(src, dst, ssem, rsem, device):
        return pltpu.make_async_remote_copy(src_ref=src, dst_ref=dst, send_sem=ssem, recv_sem=rsem, device_id={"sp": device},
                                            device_id_type=MESH)

    def landed(dst, rsem):
        remote(dst, dst, rsem, rsem, mate).wait_recv()

    def sent(src, ssem):
        remote(src, src, ssem, ssem, mate).wait_send()

    mine = pl.ds(pl.multiple_of(core * own, own), own)
    others = pl.ds(pl.multiple_of((1 - core) * own, own), own)
    own_x = pltpu.make_async_copy(x_ref, xs.at[mine], xsem.at[0])
    own_x.start()
    bar = pltpu.get_barrier_semaphore()
    peers = [mate]
    peers += [at(along(i), y, k) for i in range(1, nx) for k in range(2)]
    peers += [at(x, lax.rem(y + i, ny), core) for i in (1, ny - 1)]
    for device in peers:
        pl.semaphore_signal(bar, inc=1, device_id={"sp": device}, device_id_type=MESH)

    def fetch_kv(u):
        column = pl.ds(pl.multiple_of((2 * along(u) + core) * HEAD, HEAD), HEAD)
        for i, w_ref in enumerate((wk_ref, wv_ref)):
            pltpu.make_async_copy(w_ref.at[:, :, column], ring.at[u, :, :, pl.ds(i * HEAD, HEAD)], wsem.at[u]).start(priority=1)

    q_slabs = nx * pairs

    def q_target(t):
        return along(1 + lax.div(t, pairs))

    def fetch_q(t):
        column = ((2 * q_target(t) + core) * pairs + lax.rem(t, pairs)) * WIDE
        slot = lax.rem(nx + t, SLOTS)
        pltpu.make_async_copy(wq_ref.at[:, :, pl.ds(pl.multiple_of(column, WIDE), WIDE)], ring.at[slot], wsem.at[slot]).start(priority=1)

    for u in range(nx):
        fetch_kv(u)
    for t in range(SLOTS - nx):
        fetch_q(t)

    def wo_slab(w, i):
        return (2 * along(1 + lax.rem(w, nx)) + i) * pairs + lax.div(w, nx)

    def fetch_wo(w, i):
        slot = lax.rem(2 * w + i, WO_SLOTS)
        rows = pl.ds(pl.multiple_of(wo_slab(w, i) * WIDE, WIDE), WIDE)
        pltpu.make_async_copy(wo_ref.at[rows], wo_ring.at[slot], wosem.at[slot]).start(priority=1)

    def slab_ready(slot):
        pltpu.make_async_copy(ring.at[slot], ring.at[slot], wsem.at[slot]).wait()

    place = chip * tokens + lax.broadcasted_iota(jnp.int32, (tokens, HEAD), 0)
    angle = place.astype(F32) * turn_ref[...]
    cos_ref[...] = jnp.cos(angle)
    sin_ref[...] = jnp.where(lax.broadcasted_iota(jnp.int32, (tokens, HEAD), 1) < HEAD // 2, -1.0, 1.0) * jnp.sin(angle)
    for ref in (s0, s1, p0, p1, m0, m1, keep0, keep1, top, mix):
        ref[...] = jnp.zeros_like(ref)

    pl.semaphore_wait(bar, len(peers))
    give_x = remote(x_ref, xs.at[mine], xsem.at[1], xsem.at[2], mate)
    give_x.start()

    def norm(which):
        def rows16(r, _):
            here = pl.ds(pl.multiple_of(which * own + r * 16, 16), 16)
            wide = xs[here, :].astype(F32)
            inv = lax.rsqrt(jnp.mean(wide * wide, -1, keepdims=True) + 1e-6)
            xs[here, :] = (wide * inv * gain_ref[...].astype(F32).reshape(1, d)).astype(BF16)

        lax.fori_loop(0, own // 16, rows16, None)

    own_x.wait()
    acc[...] = xs[mine, :].astype(F32)
    norm(core)
    landed(xs.at[others], xsem.at[2])
    norm(1 - core)

    def product(slot):
        slab_ready(slot)
        return jnp.dot(xs[...], ring[slot].reshape(d, WIDE), preferred_element_type=F32).astype(BF16)

    def turned(t):
        f = t.astype(F32)
        return (f * cos_ref[...] + pltpu.roll(f, HEAD // 2, 1) * sin_ref[...]).astype(BF16)

    up, down = at(x, lax.rem(y + 1, ny), core), at(x, lax.rem(y + ny - 1, ny), core)

    def spread(block, i):
        for j, device in enumerate((up, down)):
            remote(kv_all.at[block], kv_all.at[block], nears.at[i, j], nearr.at[block], device).start()

    def row_at(i):
        return jnp.where(i == 0, x, i - 1 + ((i - 1) >= x).astype(jnp.int32))

    def forward(i):
        row = row_at(i)
        below, above = row * ny + lax.rem(y + ny - 1, ny), row * ny + lax.rem(y + 1, ny)
        landed(kv_all.at[below], nearr.at[below])
        remote(kv_all.at[below, 0], kv_all.at[below, 0], fars.at[i, 0], fark.at[row], up).start()
        landed(kv_all.at[above], nearr.at[above])
        remote(kv_all.at[above, 1], kv_all.at[above, 1], fars.at[i, 1], farv.at[row], down).start()

    def kv_turn(u, _):
        r = product(u)

        @pl.when(u + SLOTS < nx + q_slabs)
        def _():
            fetch_q(u + SLOTS - nx)

        kv_st[u, 0] = turned(r[:, :HEAD])
        kv_st[u, 1, :own] = r[:own, HEAD:].T
        kv_st[u, 1, own:] = r[own:, HEAD:].T

        @pl.when(u == 0)
        def _():
            kv_all[chip] = kv_st[0]
            spread(chip, 0)

        @pl.when(u > 0)
        def _():
            remote(kv_st.at[u], kv_all.at[chip], kvs.at[u - 1], kvr.at[u - 1], at(along(u), y, core)).start()

    lax.fori_loop(0, nx, kv_turn, None)

    def q_turn(t, _):
        r = product(lax.rem(nx + t, SLOTS))

        @pl.when(t + SLOTS < q_slabs)
        def _():
            fetch_q(t + SLOTS)

        for i in range(2):
            at_once = 2 * (t - q_slabs // 2) + i

            @pl.when((at_once >= 0) & (at_once < WO_SLOTS))
            def _():
                fetch_wo(lax.div(at_once, 2), lax.rem(at_once, 2))

        for b in range(2):
            q_st[t, pl.ds(b * tokens, tokens), :] = turned(r[:, b * HEAD : (b + 1) * HEAD])
        def send(turn):
            to = x * pairs + lax.rem(turn, pairs)

            @pl.when(turn < q_slabs - pairs)
            def _():
                remote(q_st.at[turn], q_all.at[to], qs.at[turn], qr.at[to], at(q_target(turn), y, core)).start()

            @pl.when(turn >= q_slabs - pairs)
            def _():
                q_all[to] = q_st[turn]

        def take(i):
            row = row_at(i)
            block = row * ny + y
            landed(kv_all.at[block], kvr.at[lax.rem(x - row + nx, nx) - 1])
            spread(block, i)

        @pl.when(t == 1)
        def _():
            forward(0)
            take(1)

        pl.when(t == 2)(lambda: take(2))

        @pl.when(t == 4)
        def _():
            forward(1)
            take(3)

        pl.when(t == 6)(lambda: forward(2))

        pl.when(t == 1)(lambda: send(jnp.int32(0)))
        pl.when(t >= 1)(lambda: send(t))

    lax.fori_loop(0, q_slabs, q_turn, None)

    span = 2 * tokens

    def row_of(t):
        return lax.div(t, pairs)

    def last(t):
        return lax.div(row_of(t) * ny + y, 2)

    steps = nx * pairs

    def stage(par, it, at_a, at_b, at_c):
        (ta, ka), (tb, kb), (tc, kc) = at_a, at_b, at_c
        s_new, s_old = (s0, s1)[par], (s1, s0)[par]
        m_new, m_old = (m0, m1)[par], (m1, m0)[par]
        p_new, p_old = (p0, p1)[par], (p1, p0)[par]
        keep_new, keep_old = (keep0, keep1)[par], (keep1, keep0)[par]
        tq = jnp.minimum(ta, steps - 1)
        row = row_of(tq)
        nth = row * pairs + lax.rem(tq, pairs)

        @pl.when((ka == 0) & (ta < steps))
        def _():
            pl.when(ta == 1)(lambda: forward(nx - 1))
            pl.when(row != x)(lambda: landed(q_all.at[nth], qr.at[nth]))

            @pl.when(lax.rem(ta, pairs) == 0)
            def _():
                far = row * ny + lax.rem(y + 2, ny)
                landed(kv_all.at[far, 0], fark.at[row])
                landed(kv_all.at[far, 1], farv.at[row])

        def work(masked):
            before = jnp.where(kb == 0, NEG, top[...])
            after = jnp.maximum(before, m_old[...])
            top[...] = after
            part = span // 2
            q = q_all[nth]
            most = None
            total = mix[...] * keep_old[...]
            for c in range(2):
                here = slice(c * part, (c + 1) * part)
                block, at0 = divmod(c * part, tokens)
                s = _dot(kv_all[2 * ka + block, 0, at0 : at0 + part, :], q, 1, 1)
                p_new[here] = jnp.exp2((s_old[here] - after) * e).astype(BF16)
                if (c + 1) * part % tokens == 0:
                    i = c * part // tokens
                    v = kv_all[2 * kc + i, 1]
                    v = jnp.concatenate([jnp.concatenate([v[:HEAD], v[HEAD:]], axis=1), jnp.ones((16, tokens), BF16)], axis=0)
                    total = total + _dot(v, p_old[i * tokens : (i + 1) * tokens], 1, 0)
                if masked:
                    token = lax.rem(lax.broadcasted_iota(jnp.int32, s.shape, 1), tokens)
                    gap = token - lax.broadcasted_iota(jnp.int32, s.shape, 0)
                    s = jnp.where(gap >= span * ka + c * part - tokens * (row * ny + y), s, HIDDEN)
                s_new[here] = s
                top_here = s.max(axis=0, keepdims=True)
                most = top_here if most is None else jnp.maximum(most, top_here)
            m_new[...] = most
            mix[...] = total
            keep_new[...] = jnp.exp2((before - after) * e)

        ragged = ka == last(tq)
        pl.when(ragged)(lambda: work(True))
        pl.when(jnp.logical_not(ragged))(lambda: work(False))

        @pl.when((it >= 2) & (tc < steps) & (kc == last(tc)))
        def _():
            o = (mix[:HEAD, :] * (1 / mix[HEAD : HEAD + 1, :])).T.astype(BF16)
            to, pair = row_of(tc), lax.rem(tc, pairs)
            slot = (2 * x + core) * pairs + pair
            for b in range(2):
                for h in range(2):
                    o_st[tc, b, h] = o[h * tokens + b * own : h * tokens + (b + 1) * own]
                device = at(to, y, b)

                @pl.when(device != me)
                def _():
                    remote(o_st.at[tc, b], o_all.at[slot], outs.at[tc, b], outr.at[slot], device).start()

                @pl.when(device == me)
                def _():
                    o_all[slot] = o_st[tc, b]

        return (jnp.where(ragged, ta + 1, ta), jnp.where(ragged, 0, ka + 1)), at_a, at_b

    def two(i, state):
        state = stage(0, 2 * i, *state)
        return stage(1, 2 * i + 1, *state)

    total = 2
    for t in range(steps):
        total = total + last(t) + 1
    zero = (jnp.int32(0), jnp.int32(0))
    lax.fori_loop(0, lax.div(total + 1, 2), two, (zero, zero, zero))

    for w in range(q_slabs, WO_SLOTS):
        fetch_wo(w // 2, w % 2)

    def back(w, _):
        slabs = [wo_slab(w, i) for i in range(2)]
        slots = [lax.rem(2 * w + i, WO_SLOTS) for i in range(2)]
        for i in range(2):
            pl.when((lax.rem(w, nx) != nx - 1) | (core != i))(lambda: landed(o_all.at[slabs[i]], outr.at[slabs[i]]))
        for slot in slots:
            pltpu.make_async_copy(wo_ring.at[slot], wo_ring.at[slot], wosem.at[slot]).wait()
        o = [jnp.concatenate([o_all[slab, 0], o_all[slab, 1]], axis=1) for slab in slabs]
        for j in range(d // WIDE):
            columns = slice(j * WIDE, (j + 1) * WIDE)
            acc[:, columns] += sum(jnp.dot(o[i], wo_ring[slots[i], :, columns], preferred_element_type=F32) for i in range(2))

        @pl.when(2 * w + WO_SLOTS < 2 * nx * pairs)
        def _():
            for i in range(2):
                fetch_wo(w + WO_SLOTS // 2, i)

    lax.fori_loop(0, nx * pairs, back, None)
    y_ref[...] = acc[...].astype(BF16)

    give_x.wait_send()
    for u in range(nx - 1):
        sent(kv_st.at[u + 1], kvs.at[u])
    for i in range(nx):
        for j in range(2):
            sent(kv_all.at[0], nears.at[i, j])
            sent(kv_all.at[0, 0], fars.at[i, j])
    for t in range(q_slabs - pairs):
        sent(q_st.at[t], qs.at[t])
    for t in range(steps):
        for b in range(2):
            pl.when(at(row_of(t), y, b) != me)(lambda: sent(o_st.at[t, b], outs.at[t, b]))


def solution(mesh):
    n = mesh.shape["sp"]

    def step(x, gain, wq, wk, wv, wo):
        own, d = x.shape
        chips, tokens = n // 2, 2 * own
        kv_heads = wk.shape[1] // HEAD
        half = HEAD // 2
        turn = THETA ** (-np.arange(half, dtype=np.float32) / half)
        turn = jnp.asarray(np.concatenate([turn, turn])[None], F32)
        cut = lambda w: w.reshape(d // WIDE, WIDE, w.shape[1])
        dma = pltpu.SemaphoreType.DMA
        nx = kv_heads // 2
        ny = chips // nx
        steps = n // 4
        hbm, vmem = pl.BlockSpec(memory_space=pltpu.HBM), pl.BlockSpec(memory_space=pltpu.VMEM)
        return pl.pallas_call(
            functools.partial(_kernel, n, kv_heads),
            out_shape=jax.ShapeDtypeStruct((own, d), BF16),
            in_specs=[hbm, vmem, vmem, hbm, hbm, hbm, hbm],
            out_specs=vmem,
            scratch_shapes=[
                *[pltpu.VMEM((tokens, HEAD), F32)] * 2,
                pltpu.VMEM((tokens, d), BF16),
                pltpu.VMEM((SLOTS, d // WIDE, WIDE, WIDE), BF16),
                pltpu.VMEM((WO_SLOTS, WIDE, d), BF16),
                pltpu.VMEM((nx, 2, tokens, HEAD), BF16),
                pltpu.VMEM((steps, 2 * tokens, HEAD), BF16),
                pltpu.VMEM((chips, 2, tokens, HEAD), BF16),
                pltpu.VMEM((steps, 2 * tokens, HEAD), BF16),
                pltpu.VMEM((steps, 2, 2, own, HEAD), BF16),
                pltpu.VMEM((n // 2, 2, own, HEAD), BF16),
                pltpu.VMEM((own, d), F32),
                *[pltpu.VMEM((2 * tokens, 2 * tokens), F32)] * 2,
                *[pltpu.VMEM((2 * tokens, 2 * tokens), BF16)] * 2,
                *[pltpu.VMEM((1, 2 * tokens), F32)] * 5,
                pltpu.VMEM((HEAD + 16, 2 * tokens), F32),
                dma((SLOTS,)), dma((WO_SLOTS,)), dma((3,)), dma((nx - 1,)), dma((nx - 1,)), dma((nx, 2)), dma((chips,)), dma((nx, 2)), dma((nx,)), dma((nx,)),
                dma((steps,)), dma((steps,)), dma((steps, 2)), dma((n // 2,)),
            ],
            compiler_params=pltpu.CompilerParams(collective_id=0, has_side_effects=True, vmem_limit_bytes=67043328),
        )(x, gain, turn, cut(wq), cut(wk), cut(wv), wo)

    tokens, whole = P(("dp", "sp"), None), P(None, None)
    return jax.shard_map(
        step,
        mesh=mesh,
        in_specs=(tokens, P(None), whole, whole, whole, whole),
        out_specs=tokens,
        check_vma=False,
    )
```

```python
import functools

import jax
import jax.numpy as jnp
import numpy as np
from jax import lax
from jax.experimental import pallas as pl
from jax.experimental.pallas import tpu as pltpu
from jax.sharding import PartitionSpec as P

HEAD = 128
THETA = 10000
NEG = -1e30
HIDDEN = 2 * NEG
LOG2E = 1.4426950408889634
WIDE = 256
SLOTS = 5
WO_SLOTS = 10
MESH = pl.DeviceIdType.MESH
F32, BF16 = jnp.float32, jnp.bfloat16


def _dot(a, b, ca, cb):
    return lax.dot_general(a, b, (((ca,), (cb,)), ((), ())), preferred_element_type=F32)


def _kernel(n, kv_heads, x_ref, gain_ref, turn_ref, wq_ref, wk_ref, wv_ref, wo_ref, y_ref,
            cos_ref, sin_ref, gain_s, xs, ring, wo_ring, kv_st, q_st, kv_all, q_all, o_st, o_all, acc, s0, s1, p0, p1, m0, m1, keep0, keep1, top, mix,
            y_s, wsem, wosem, ysem, xsem, kvs, kvr, nears, nearr, fars, fark, farv, qs, qr, outs, outr):
    own, d = x_ref.shape
    chips, tokens = n // 2, 2 * own
    slices = d // WIDE
    nx = kv_heads // 2
    ny = chips // nx
    pairs = n // kv_heads // 2
    me = lax.axis_index("sp")
    chip, core = lax.div(me, 2), lax.rem(me, 2)
    x, y = lax.div(chip, ny), lax.rem(chip, ny)
    mate = me + 1 - 2 * core
    scale = HEAD**-0.5
    e = scale * LOG2E

    def at(i, j, k):
        return (i * ny + j) * 2 + k

    def along(i):
        return lax.rem(x + i, nx)

    def remote(src, dst, ssem, rsem, device):
        return pltpu.make_async_remote_copy(src_ref=src, dst_ref=dst, send_sem=ssem, recv_sem=rsem, device_id={"sp": device},
                                            device_id_type=MESH)

    def landed(dst, rsem):
        remote(dst, dst, rsem, rsem, mate).wait_recv()

    def sent(src, ssem):
        remote(src, src, ssem, ssem, mate).wait_send()

    mine = pl.ds(pl.multiple_of(core * own, own), own)
    others = pl.ds(pl.multiple_of((1 - core) * own, own), own)
    own_x = pltpu.make_async_copy(x_ref, xs.at[mine], xsem.at[0])
    own_x.start()
    bar = pltpu.get_barrier_semaphore()
    peers = [mate]
    peers += [at(along(i), y, k) for i in range(1, nx) for k in range(2)]
    peers += [at(x, lax.rem(y + i, ny), core) for i in (1, ny - 1)]
    for device in peers:
        pl.semaphore_signal(bar, inc=1, device_id={"sp": device}, device_id_type=MESH)

    def fetch_kv(u):
        column = pl.ds(pl.multiple_of((2 * along(u) + core) * HEAD, HEAD), HEAD)
        for i, w_ref in enumerate((wk_ref, wv_ref)):
            pltpu.make_async_copy(w_ref.at[:, :, column], ring.at[u, :, :, pl.ds(i * HEAD, HEAD)], wsem.at[u]).start(priority=1)

    q_slabs = steps = nx * pairs

    def q_target(t):
        return along(1 + lax.div(t, pairs))

    def fetch_q(t):
        column = ((2 * q_target(t) + core) * pairs + lax.rem(t, pairs)) * WIDE
        slot = lax.rem(nx + t, SLOTS)
        pltpu.make_async_copy(wq_ref.at[:, :, pl.ds(pl.multiple_of(column, WIDE), WIDE)], ring.at[slot], wsem.at[slot]).start(priority=1)

    for u in range(nx):
        fetch_kv(u)
    for t in range(SLOTS - nx):
        fetch_q(t)

    def wo_slab(w, i):
        return (2 * along(1 + lax.rem(w, nx)) + i) * pairs + lax.div(w, nx)

    def fetch_wo(w, i):
        slot = lax.rem(2 * w + i, WO_SLOTS)
        rows = pl.ds(pl.multiple_of(wo_slab(w, i) * WIDE, WIDE), WIDE)
        pltpu.make_async_copy(wo_ref.at[rows], wo_ring.at[slot], wosem.at[slot]).start(priority=1)

    def slab_ready(slot):
        pltpu.make_async_copy(ring.at[slot], ring.at[slot], wsem.at[slot]).wait()

    gain_s[...] = gain_ref[...].astype(F32).reshape(1, d)
    place = chip * tokens + lax.broadcasted_iota(jnp.int32, (tokens, HEAD), 0)
    angle = place.astype(F32) * turn_ref[...]
    cos_ref[...] = jnp.cos(angle)
    sin_ref[...] = jnp.where(lax.broadcasted_iota(jnp.int32, (tokens, HEAD), 1) < HEAD // 2, -1.0, 1.0) * jnp.sin(angle)
    for ref in (s0, s1, p0, p1, m0, m1, keep0, keep1, top, mix):
        ref[...] = jnp.zeros_like(ref)

    pl.semaphore_wait(bar, len(peers))
    give_x = remote(x_ref, xs.at[mine], xsem.at[1], xsem.at[2], mate)
    give_x.start()

    def norm(which):
        def some(r, _):
            here = pl.ds(pl.multiple_of(which * own + r * 32, 32), 32)
            wide = xs[here, :].astype(F32)
            inv = lax.rsqrt(jnp.mean(wide * wide, -1, keepdims=True) + 1e-6)
            xs[here, :] = (wide * inv * gain_s[...]).astype(BF16)

        lax.fori_loop(0, own // 32, some, None)

    own_x.wait()
    acc[...] = xs[mine, :].astype(F32)
    norm(core)
    landed(xs.at[others], xsem.at[2])
    norm(1 - core)

    def product(slot):
        slab_ready(slot)
        return jnp.dot(xs[...], ring[slot].reshape(d, WIDE), preferred_element_type=F32).astype(BF16)

    def turned(t):
        f = t.astype(F32)
        return (f * cos_ref[...] + pltpu.roll(f, HEAD // 2, 1) * sin_ref[...]).astype(BF16)

    up, down = at(x, lax.rem(y + 1, ny), core), at(x, lax.rem(y + ny - 1, ny), core)

    def spread(block, i):
        for j, device in enumerate((up, down)):
            remote(kv_all.at[block], kv_all.at[block], nears.at[i, j], nearr.at[block], device).start()

    def row_at(i):
        return jnp.where(i == 0, x, i - 1 + ((i - 1) >= x).astype(jnp.int32))

    def forward(i):
        row = row_at(i)
        below, above = row * ny + lax.rem(y + ny - 1, ny), row * ny + lax.rem(y + 1, ny)
        landed(kv_all.at[below], nearr.at[below])
        remote(kv_all.at[below, 0], kv_all.at[below, 0], fars.at[i, 0], fark.at[row], up).start()
        landed(kv_all.at[above], nearr.at[above])
        remote(kv_all.at[above, 1], kv_all.at[above, 1], fars.at[i, 1], farv.at[row], down).start()

    def kv_turn(u, _):
        r = product(u)

        @pl.when(u + SLOTS < nx + q_slabs)
        def _():
            fetch_q(u + SLOTS - nx)

        kv_st[u, 0] = turned(r[:, :HEAD])
        kv_st[u, 1, :own] = r[:own, HEAD:].T
        kv_st[u, 1, own:] = r[own:, HEAD:].T

        @pl.when(u == 0)
        def _():
            kv_all[chip] = kv_st[0]
            spread(chip, 0)

        @pl.when(u > 0)
        def _():
            remote(kv_st.at[u], kv_all.at[chip], kvs.at[u - 1], kvr.at[u - 1], at(along(u), y, core)).start()

    lax.fori_loop(0, nx, kv_turn, None)

    def q_turn(t, _):
        r = product(lax.rem(nx + t, SLOTS))

        @pl.when(t + SLOTS < q_slabs)
        def _():
            fetch_q(t + SLOTS)

        for i in range(2):
            at_once = 2 * (t - q_slabs // 2) + i

            @pl.when((at_once >= 0) & (at_once < WO_SLOTS))
            def _():
                fetch_wo(lax.div(at_once, 2), lax.rem(at_once, 2))

        for b in range(2):
            q_st[t, :, b * tokens : (b + 1) * tokens] = turned(r[:, b * HEAD : (b + 1) * HEAD]).T
        def send(turn):
            to = x * pairs + lax.rem(turn, pairs)

            @pl.when(turn < q_slabs - pairs)
            def _():
                remote(q_st.at[turn], q_all.at[to], qs.at[turn], qr.at[to], at(q_target(turn), y, core)).start()

            @pl.when(turn >= q_slabs - pairs)
            def _():
                q_all[to] = q_st[turn]

        def take(i):
            row = row_at(i)
            block = row * ny + y
            landed(kv_all.at[block], kvr.at[lax.rem(x - row + nx, nx) - 1])
            spread(block, i)

        @pl.when(t == 1)
        def _():
            forward(0)
            take(1)

        pl.when(t == 2)(lambda: take(2))

        @pl.when(t == 4)
        def _():
            forward(1)
            take(3)

        pl.when(t == 6)(lambda: forward(2))

        pl.when(t == 1)(lambda: send(jnp.int32(0)))
        pl.when(t >= 1)(lambda: send(t))

    lax.fori_loop(0, q_slabs, q_turn, None)

    span = 2 * tokens

    def row_of(t):
        return jnp.where(t < steps - 3, lax.div(t, pairs), jnp.where(t == steps - 1, nx - 2, nx - 1))

    def pair_of(t):
        return jnp.where(t < steps - 3, lax.rem(t, pairs), jnp.where(t == steps - 3, 0, pairs - 1))

    def last(t):
        return lax.div(row_of(t) * ny + y, 2)


    def stage(par, it, at_a, at_b, at_c):
        (ta, ka), (tb, kb), (tc, kc) = at_a, at_b, at_c
        s_new, s_old = (s0, s1)[par], (s1, s0)[par]
        m_new, m_old = (m0, m1)[par], (m1, m0)[par]
        p_new, p_old = (p0, p1)[par], (p1, p0)[par]
        keep_new, keep_old = (keep0, keep1)[par], (keep1, keep0)[par]
        tq = jnp.minimum(ta, steps - 1)
        row = row_of(tq)
        nth = row * pairs + pair_of(tq)

        @pl.when((ka == 0) & (ta < steps))
        def _():
            pl.when(ta == 1)(lambda: forward(nx - 1))
            pl.when(row != x)(lambda: landed(q_all.at[nth], qr.at[nth]))

            @pl.when(pair_of(ta) == 0)
            def _():
                far = row * ny + lax.rem(y + 2, ny)
                landed(kv_all.at[far, 0], fark.at[row])
                landed(kv_all.at[far, 1], farv.at[row])

        def work(masked):
            before = jnp.where(kb == 0, NEG, top[...])
            after = jnp.maximum(before, m_old[...])
            top[...] = after
            part = span // 2
            q = q_all[nth]
            most = None
            total = mix[...] * keep_old[...]
            for c in range(2):
                here = slice(c * part, (c + 1) * part)
                block, at0 = divmod(c * part, tokens)
                s = _dot(kv_all[2 * ka + block, 0, at0 : at0 + part, :], q, 1, 0)
                p_new[here] = jnp.exp2((s_old[here] - after) * e).astype(BF16)
                if (c + 1) * part % tokens == 0:
                    i = c * part // tokens
                    v = kv_all[2 * kc + i, 1]
                    v = jnp.concatenate([jnp.concatenate([v[:HEAD], v[HEAD:]], axis=1), jnp.ones((16, tokens), BF16)], axis=0)
                    total = total + _dot(v, p_old[i * tokens : (i + 1) * tokens], 1, 0)
                if masked:
                    token = lax.rem(lax.broadcasted_iota(jnp.int32, s.shape, 1), tokens)
                    gap = token - lax.broadcasted_iota(jnp.int32, s.shape, 0)
                    s = jnp.where(gap >= span * ka + c * part - tokens * (row * ny + y), s, HIDDEN)
                s_new[here] = s
                top_here = s.max(axis=0, keepdims=True)
                most = top_here if most is None else jnp.maximum(most, top_here)
            m_new[...] = most
            mix[...] = total
            keep_new[...] = jnp.exp2((before - after) * e)

        ragged = ka == last(tq)
        pl.when(ragged)(lambda: work(True))
        pl.when(jnp.logical_not(ragged))(lambda: work(False))

        @pl.when((it >= 2) & (tc < steps) & (kc == last(tc)))
        def _():
            o = (mix[:HEAD, :] * (1 / mix[HEAD : HEAD + 1, :])).T.astype(BF16)
            to, pair = row_of(tc), pair_of(tc)
            slot = (2 * x + core) * pairs + pair
            for b in range(2):
                for h in range(2):
                    o_st[tc, b, h] = o[h * tokens + b * own : h * tokens + (b + 1) * own]
                device = at(to, y, b)

                @pl.when(device != me)
                def _():
                    remote(o_st.at[tc, b], o_all.at[slot], outs.at[tc, b], outr.at[slot], device).start()

                @pl.when(device == me)
                def _():
                    o_all[slot] = o_st[tc, b]

        return (jnp.where(ragged, ta + 1, ta), jnp.where(ragged, 0, ka + 1)), at_a, at_b

    def two(i, state):
        state = stage(0, 2 * i, *state)
        return stage(1, 2 * i + 1, *state)

    total = 2
    for t in range(steps):
        total = total + last(t) + 1
    zero = (jnp.int32(0), jnp.int32(0))
    lax.fori_loop(0, lax.div(total + 1, 2), two, (zero, zero, zero))

    for w in range(q_slabs, WO_SLOTS):
        fetch_wo(w // 2, w % 2)

    def back(w, final):
        slabs = [wo_slab(w, i) for i in range(2)]
        slots = [lax.rem(2 * w + i, WO_SLOTS) for i in range(2)]
        for i in range(2):
            pl.when((lax.rem(w, nx) != nx - 1) | (core != i))(lambda: landed(o_all.at[slabs[i]], outr.at[slabs[i]]))
        for slot in slots:
            pltpu.make_async_copy(wo_ring.at[slot], wo_ring.at[slot], wosem.at[slot]).wait()
        o = [jnp.concatenate([o_all[slab, 0], o_all[slab, 1]], axis=1) for slab in slabs]
        for j in range(d // WIDE):
            columns = slice(j * WIDE, (j + 1) * WIDE)
            part = sum(jnp.dot(o[i], wo_ring[slots[i], :, columns], preferred_element_type=F32) for i in range(2))
            if final:
                y_s[:, columns] = (acc[:, columns] + part).astype(BF16)
                pltpu.make_async_copy(y_s.at[:, pl.ds(j * WIDE, WIDE)], y_ref.at[:, pl.ds(j * WIDE, WIDE)], ysem).start()
            else:
                acc[:, columns] += part

        @pl.when(2 * w + WO_SLOTS < 2 * nx * pairs)
        def _():
            for i in range(2):
                fetch_wo(w + WO_SLOTS // 2, i)

    lax.fori_loop(0, nx * pairs - 1, lambda w, _: back(w, False), None)
    back(jnp.int32(nx * pairs - 1), True)

    give_x.wait_send()
    for u in range(nx - 1):
        sent(kv_st.at[u + 1], kvs.at[u])
    for i in range(nx):
        for j in range(2):
            sent(kv_all.at[0], nears.at[i, j])
            sent(kv_all.at[0, 0], fars.at[i, j])
    for t in range(q_slabs - pairs):
        sent(q_st.at[t], qs.at[t])
    for t in range(steps):
        for b in range(2):
            pl.when(at(row_of(t), y, b) != me)(lambda: sent(o_st.at[t, b], outs.at[t, b]))
    pltpu.make_async_copy(y_s, y_ref, ysem).wait()


def solution(mesh):
    n = mesh.shape["sp"]

    def step(x, gain, wq, wk, wv, wo):
        own, d = x.shape
        chips, tokens = n // 2, 2 * own
        kv_heads = wk.shape[1] // HEAD
        half = HEAD // 2
        turn = THETA ** (-np.arange(half, dtype=np.float32) / half)
        turn = jnp.asarray(np.concatenate([turn, turn])[None], F32)
        cut = lambda w: w.reshape(d // WIDE, WIDE, w.shape[1])
        dma = pltpu.SemaphoreType.DMA
        nx = kv_heads // 2
        ny = chips // nx
        steps = n // 4
        hbm, vmem = pl.BlockSpec(memory_space=pltpu.HBM), pl.BlockSpec(memory_space=pltpu.VMEM)
        return pl.pallas_call(
            functools.partial(_kernel, n, kv_heads),
            out_shape=jax.ShapeDtypeStruct((own, d), BF16),
            in_specs=[hbm, vmem, vmem, hbm, hbm, hbm, hbm],
            out_specs=hbm,
            scratch_shapes=[
                *[pltpu.VMEM((tokens, HEAD), F32)] * 2,
                pltpu.VMEM((1, d), F32),
                pltpu.VMEM((tokens, d), BF16),
                pltpu.VMEM((SLOTS, d // WIDE, WIDE, WIDE), BF16),
                pltpu.VMEM((WO_SLOTS, WIDE, d), BF16),
                pltpu.VMEM((nx, 2, tokens, HEAD), BF16),
                pltpu.VMEM((steps, HEAD, 2 * tokens), BF16),
                pltpu.VMEM((chips, 2, tokens, HEAD), BF16),
                pltpu.VMEM((steps, HEAD, 2 * tokens), BF16),
                pltpu.VMEM((steps, 2, 2, own, HEAD), BF16),
                pltpu.VMEM((n // 2, 2, own, HEAD), BF16),
                pltpu.VMEM((own, d), F32),
                *[pltpu.VMEM((2 * tokens, 2 * tokens), F32)] * 2,
                *[pltpu.VMEM((2 * tokens, 2 * tokens), BF16)] * 2,
                *[pltpu.VMEM((1, 2 * tokens), F32)] * 5,
                pltpu.VMEM((HEAD + 16, 2 * tokens), F32),
                pltpu.VMEM((own, d), BF16),
                dma((SLOTS,)), dma((WO_SLOTS,)), dma(()), dma((3,)), dma((nx - 1,)), dma((nx - 1,)), dma((nx, 2)), dma((chips,)), dma((nx, 2)), dma((nx,)), dma((nx,)),
                dma((steps,)), dma((steps,)), dma((steps, 2)), dma((n // 2,)),
            ],
            compiler_params=pltpu.CompilerParams(collective_id=0, has_side_effects=True, vmem_limit_bytes=67043328),
        )(x, gain, turn, cut(wq), cut(wk), cut(wv), wo)

    tokens, whole = P(("dp", "sp"), None), P(None, None)
    return jax.shard_map(
        step,
        mesh=mesh,
        in_specs=(tokens, P(None), whole, whole, whole, whole),
        out_specs=tokens,
        check_vma=False,
    )
```

```python
import functools

import jax
import jax.numpy as jnp
import numpy as np
from jax import lax
from jax.experimental import pallas as pl
from jax.experimental.pallas import tpu as pltpu
from jax.sharding import PartitionSpec as P

HEAD = 128
THETA = 10000
NEG = -1e30
HIDDEN = 2 * NEG
LOG2E = 1.4426950408889634
WIDE = 256
SLOTS = 5
WO_SLOTS = 10
MESH = pl.DeviceIdType.MESH
F32, BF16 = jnp.float32, jnp.bfloat16


def _dot(a, b, ca, cb):
    return lax.dot_general(a, b, (((ca,), (cb,)), ((), ())), preferred_element_type=F32)


def _kernel(n, kv_heads, x_ref, gain_ref, turn_ref, wq_ref, wk_ref, wv_ref, wo_ref, y_ref,
            cos_ref, sin_ref, gain_s, xs, ring, wo_ring, kv_st, q_st, kv_all, q_all, o_st, o_all, acc, s0, s1, p0, p1, m0, m1, keep0, keep1, top, mix,
            y_s, wsem, wosem, ysem, xsem, kvs, kvr, nears, nearr, fars, fark, farv, qs, qr, outs, outr):
    own, d = x_ref.shape
    chips, tokens = n // 2, 2 * own
    slices = d // WIDE
    nx = kv_heads // 2
    ny = chips // nx
    pairs = n // kv_heads // 2
    me = lax.axis_index("sp")
    chip, core = lax.div(me, 2), lax.rem(me, 2)
    x, y = lax.div(chip, ny), lax.rem(chip, ny)
    mate = me + 1 - 2 * core
    scale = HEAD**-0.5
    e = scale * LOG2E

    def at(i, j, k):
        return (i * ny + j) * 2 + k

    def along(i):
        return lax.rem(x + i, nx)

    def remote(src, dst, ssem, rsem, device):
        return pltpu.make_async_remote_copy(src_ref=src, dst_ref=dst, send_sem=ssem, recv_sem=rsem, device_id={"sp": device},
                                            device_id_type=MESH)

    def landed(dst, rsem):
        remote(dst, dst, rsem, rsem, mate).wait_recv()

    def sent(src, ssem):
        remote(src, src, ssem, ssem, mate).wait_send()

    mine = pl.ds(pl.multiple_of(core * own, own), own)
    others = pl.ds(pl.multiple_of((1 - core) * own, own), own)
    own_x = pltpu.make_async_copy(x_ref, xs.at[mine], xsem.at[0])
    own_x.start()
    bar = pltpu.get_barrier_semaphore()
    peers = [mate]
    peers += [at(along(i), y, k) for i in range(1, nx) for k in range(2)]
    peers += [at(x, lax.rem(y + i, ny), core) for i in (1, ny - 1)]
    for device in peers:
        pl.semaphore_signal(bar, inc=1, device_id={"sp": device}, device_id_type=MESH)

    def fetch_kv(u):
        column = pl.ds(pl.multiple_of((2 * along(nx - u) + core) * HEAD, HEAD), HEAD)
        for i, w_ref in enumerate((wk_ref, wv_ref)):
            pltpu.make_async_copy(w_ref.at[:, :, column], ring.at[u, :, :, pl.ds(i * HEAD, HEAD)], wsem.at[u]).start(priority=1)

    q_slabs = steps = nx * pairs

    def q_target(t):
        return along(nx - 1 - lax.div(t, pairs))

    def fetch_q(t):
        column = ((2 * q_target(t) + core) * pairs + lax.rem(t, pairs)) * WIDE
        slot = lax.rem(nx + t, SLOTS)
        pltpu.make_async_copy(wq_ref.at[:, :, pl.ds(pl.multiple_of(column, WIDE), WIDE)], ring.at[slot], wsem.at[slot]).start(priority=1)

    for u in range(nx):
        fetch_kv(u)
    for t in range(SLOTS - nx):
        fetch_q(t)

    def wo_slab(w, i):
        return (2 * along(1 + lax.rem(w, nx)) + i) * pairs + lax.div(w, nx)

    def fetch_wo(w, i):
        slot = lax.rem(2 * w + i, WO_SLOTS)
        rows = pl.ds(pl.multiple_of(wo_slab(w, i) * WIDE, WIDE), WIDE)
        pltpu.make_async_copy(wo_ref.at[rows], wo_ring.at[slot], wosem.at[slot]).start(priority=1)

    def slab_ready(slot):
        pltpu.make_async_copy(ring.at[slot], ring.at[slot], wsem.at[slot]).wait()

    gain_s[...] = gain_ref[...].astype(F32).reshape(1, d)
    place = chip * tokens + lax.broadcasted_iota(jnp.int32, (tokens, HEAD), 0)
    angle = place.astype(F32) * turn_ref[...]
    cos_ref[...] = jnp.cos(angle)
    sin_ref[...] = jnp.where(lax.broadcasted_iota(jnp.int32, (tokens, HEAD), 1) < HEAD // 2, -1.0, 1.0) * jnp.sin(angle)
    for ref in (s0, s1, p0, p1, m0, m1, keep0, keep1, top, mix):
        ref[...] = jnp.zeros_like(ref)

    pl.semaphore_wait(bar, len(peers))
    give_x = remote(x_ref, xs.at[mine], xsem.at[1], xsem.at[2], mate)
    give_x.start()

    def norm(which):
        def some(r, _):
            here = pl.ds(pl.multiple_of(which * own + r * 32, 32), 32)
            wide = xs[here, :].astype(F32)
            inv = lax.rsqrt(jnp.mean(wide * wide, -1, keepdims=True) + 1e-6)
            xs[here, :] = (wide * inv * gain_s[...]).astype(BF16)

        lax.fori_loop(0, own // 32, some, None)

    own_x.wait()
    acc[...] = xs[mine, :].astype(F32)
    norm(core)
    landed(xs.at[others], xsem.at[2])
    norm(1 - core)

    def product(slot):
        slab_ready(slot)
        return jnp.dot(xs[...], ring[slot].reshape(d, WIDE), preferred_element_type=F32).astype(BF16)

    def turned(t):
        f = t.astype(F32)
        return (f * cos_ref[...] + pltpu.roll(f, HEAD // 2, 1) * sin_ref[...]).astype(BF16)

    up, down = at(x, lax.rem(y + 1, ny), core), at(x, lax.rem(y + ny - 1, ny), core)

    def spread(block, i):
        for j, device in enumerate((up, down)):
            remote(kv_all.at[block], kv_all.at[block], nears.at[i, j], nearr.at[block], device).start()

    def row_at(i):
        return jnp.where(i == 0, x, i - 1 + ((i - 1) >= x).astype(jnp.int32))

    def forward(i):
        row = row_at(i)
        below, above = row * ny + lax.rem(y + ny - 1, ny), row * ny + lax.rem(y + 1, ny)
        landed(kv_all.at[below], nearr.at[below])
        remote(kv_all.at[below, 0], kv_all.at[below, 0], fars.at[i, 0], fark.at[row], up).start()
        landed(kv_all.at[above], nearr.at[above])
        remote(kv_all.at[above, 1], kv_all.at[above, 1], fars.at[i, 1], farv.at[row], down).start()

    def kv_turn(u, _):
        r = product(u)

        @pl.when(u + SLOTS < nx + q_slabs)
        def _():
            fetch_q(u + SLOTS - nx)

        kv_st[u, 0] = turned(r[:, :HEAD])
        kv_st[u, 1, :own] = r[:own, HEAD:].T
        kv_st[u, 1, own:] = r[own:, HEAD:].T

        @pl.when(u == 0)
        def _():
            kv_all[chip] = kv_st[0]
            spread(chip, 0)

        @pl.when(u > 0)
        def _():
            remote(kv_st.at[u], kv_all.at[chip], kvs.at[u - 1], kvr.at[u - 1], at(along(nx - u), y, core)).start()

    lax.fori_loop(0, nx, kv_turn, None)

    def q_turn(t, _):
        r = product(lax.rem(nx + t, SLOTS))

        @pl.when(t + SLOTS < q_slabs)
        def _():
            fetch_q(t + SLOTS)

        for i in range(2):
            at_once = 2 * (t - q_slabs // 2) + i

            @pl.when((at_once >= 0) & (at_once < WO_SLOTS))
            def _():
                fetch_wo(lax.div(at_once, 2), lax.rem(at_once, 2))

        for b in range(2):
            q_st[t, :, b * tokens : (b + 1) * tokens] = turned(r[:, b * HEAD : (b + 1) * HEAD]).T
        def send(turn):
            to = x * pairs + lax.rem(turn, pairs)

            @pl.when(turn < q_slabs - pairs)
            def _():
                remote(q_st.at[turn], q_all.at[to], qs.at[turn], qr.at[to], at(q_target(turn), y, core)).start()

            @pl.when(turn >= q_slabs - pairs)
            def _():
                q_all[to] = q_st[turn]

        def take(i):
            row = row_at(i)
            block = row * ny + y
            landed(kv_all.at[block], kvr.at[lax.rem(row - x + nx, nx) - 1])
            spread(block, i)

        @pl.when(t == 1)
        def _():
            forward(0)
            take(1)

        pl.when(t == 2)(lambda: take(2))

        @pl.when(t == 4)
        def _():
            forward(1)
            take(3)

        pl.when(t == 6)(lambda: forward(2))

        send(t)

    lax.fori_loop(0, q_slabs, q_turn, None)

    span = 2 * tokens

    def row_of(t):
        return jnp.where(t < steps - 3, lax.div(t, pairs), jnp.where(t == steps - 1, nx - 2, nx - 1))

    def pair_of(t):
        return jnp.where(t < steps - 3, lax.rem(t, pairs), jnp.where(t == steps - 3, 0, pairs - 1))

    def last(t):
        return lax.div(row_of(t) * ny + y, 2)


    def stage(par, it, at_a, at_b, at_c):
        (ta, ka), (tb, kb), (tc, kc) = at_a, at_b, at_c
        s_new, s_old = (s0, s1)[par], (s1, s0)[par]
        m_new, m_old = (m0, m1)[par], (m1, m0)[par]
        p_new, p_old = (p0, p1)[par], (p1, p0)[par]
        keep_new, keep_old = (keep0, keep1)[par], (keep1, keep0)[par]
        tq = jnp.minimum(ta, steps - 1)
        row = row_of(tq)
        nth = row * pairs + pair_of(tq)

        @pl.when((ka == 0) & (ta < steps))
        def _():
            pl.when(ta == 1)(lambda: forward(nx - 1))
            pl.when(row != x)(lambda: landed(q_all.at[nth], qr.at[nth]))

            @pl.when(pair_of(ta) == 0)
            def _():
                far = row * ny + lax.rem(y + 2, ny)
                landed(kv_all.at[far, 0], fark.at[row])
                landed(kv_all.at[far, 1], farv.at[row])

        def work(masked):
            before = jnp.where(kb == 0, NEG, top[...])
            after = jnp.maximum(before, m_old[...])
            top[...] = after
            part = span // 2
            q = q_all[nth]
            most = None
            total = mix[...] * keep_old[...]
            for c in range(2):
                here = slice(c * part, (c + 1) * part)
                block, at0 = divmod(c * part, tokens)
                s = _dot(kv_all[2 * ka + block, 0, at0 : at0 + part, :], q, 1, 0)
                p_new[here] = jnp.exp2((s_old[here] - after) * e).astype(BF16)
                if (c + 1) * part % tokens == 0:
                    i = c * part // tokens
                    v = kv_all[2 * kc + i, 1]
                    v = jnp.concatenate([jnp.concatenate([v[:HEAD], v[HEAD:]], axis=1), jnp.ones((16, tokens), BF16)], axis=0)
                    total = total + _dot(v, p_old[i * tokens : (i + 1) * tokens], 1, 0)
                if masked:
                    token = lax.rem(lax.broadcasted_iota(jnp.int32, s.shape, 1), tokens)
                    gap = token - lax.broadcasted_iota(jnp.int32, s.shape, 0)
                    s = jnp.where(gap >= span * ka + c * part - tokens * (row * ny + y), s, HIDDEN)
                s_new[here] = s
                top_here = s.max(axis=0, keepdims=True)
                most = top_here if most is None else jnp.maximum(most, top_here)
            m_new[...] = most
            mix[...] = total
            keep_new[...] = jnp.exp2((before - after) * e)

        ragged = ka == last(tq)
        pl.when(ragged)(lambda: work(True))
        pl.when(jnp.logical_not(ragged))(lambda: work(False))

        @pl.when((it >= 2) & (tc < steps) & (kc == last(tc)))
        def _():
            o = (mix[:HEAD, :] * (1 / mix[HEAD : HEAD + 1, :])).T.astype(BF16)
            to, pair = row_of(tc), pair_of(tc)
            slot = (2 * x + core) * pairs + pair
            for b in range(2):
                for h in range(2):
                    o_st[tc, b, h] = o[h * tokens + b * own : h * tokens + (b + 1) * own]
                device = at(to, y, b)

                @pl.when(device != me)
                def _():
                    remote(o_st.at[tc, b], o_all.at[slot], outs.at[tc, b], outr.at[slot], device).start()

                @pl.when(device == me)
                def _():
                    o_all[slot] = o_st[tc, b]

        return (jnp.where(ragged, ta + 1, ta), jnp.where(ragged, 0, ka + 1)), at_a, at_b

    def two(i, state):
        state = stage(0, 2 * i, *state)
        return stage(1, 2 * i + 1, *state)

    total = 2
    for t in range(steps):
        total = total + last(t) + 1
    zero = (jnp.int32(0), jnp.int32(0))
    lax.fori_loop(0, lax.div(total + 1, 2), two, (zero, zero, zero))

    for w in range(q_slabs, WO_SLOTS):
        fetch_wo(w // 2, w % 2)

    def back(w, final):
        slabs = [wo_slab(w, i) for i in range(2)]
        slots = [lax.rem(2 * w + i, WO_SLOTS) for i in range(2)]
        for i in range(2):
            pl.when((lax.rem(w, nx) != nx - 1) | (core != i))(lambda: landed(o_all.at[slabs[i]], outr.at[slabs[i]]))
        for slot in slots:
            pltpu.make_async_copy(wo_ring.at[slot], wo_ring.at[slot], wosem.at[slot]).wait()
        o = [jnp.concatenate([o_all[slab, 0], o_all[slab, 1]], axis=1) for slab in slabs]
        for j in range(d // WIDE):
            columns = slice(j * WIDE, (j + 1) * WIDE)
            part = sum(jnp.dot(o[i], wo_ring[slots[i], :, columns], preferred_element_type=F32) for i in range(2))
            if final:
                y_s[:, columns] = (acc[:, columns] + part).astype(BF16)
                pltpu.make_async_copy(y_s.at[:, pl.ds(j * WIDE, WIDE)], y_ref.at[:, pl.ds(j * WIDE, WIDE)], ysem).start()
            else:
                acc[:, columns] += part

        @pl.when(2 * w + WO_SLOTS < 2 * nx * pairs)
        def _():
            for i in range(2):
                fetch_wo(w + WO_SLOTS // 2, i)

    lax.fori_loop(0, nx * pairs - 1, lambda w, _: back(w, False), None)
    back(jnp.int32(nx * pairs - 1), True)

    give_x.wait_send()
    for u in range(nx - 1):
        sent(kv_st.at[u + 1], kvs.at[u])
    for i in range(nx):
        for j in range(2):
            sent(kv_all.at[0], nears.at[i, j])
            sent(kv_all.at[0, 0], fars.at[i, j])
    for t in range(q_slabs - pairs):
        sent(q_st.at[t], qs.at[t])
    for t in range(steps):
        for b in range(2):
            pl.when(at(row_of(t), y, b) != me)(lambda: sent(o_st.at[t, b], outs.at[t, b]))
    pltpu.make_async_copy(y_s, y_ref, ysem).wait()


def solution(mesh):
    n = mesh.shape["sp"]

    def step(x, gain, wq, wk, wv, wo):
        own, d = x.shape
        chips, tokens = n // 2, 2 * own
        kv_heads = wk.shape[1] // HEAD
        half = HEAD // 2
        turn = THETA ** (-np.arange(half, dtype=np.float32) / half)
        turn = jnp.asarray(np.concatenate([turn, turn])[None], F32)
        cut = lambda w: w.reshape(d // WIDE, WIDE, w.shape[1])
        dma = pltpu.SemaphoreType.DMA
        nx = kv_heads // 2
        ny = chips // nx
        steps = n // 4
        hbm, vmem = pl.BlockSpec(memory_space=pltpu.HBM), pl.BlockSpec(memory_space=pltpu.VMEM)
        return pl.pallas_call(
            functools.partial(_kernel, n, kv_heads),
            out_shape=jax.ShapeDtypeStruct((own, d), BF16),
            in_specs=[hbm, vmem, vmem, hbm, hbm, hbm, hbm],
            out_specs=hbm,
            scratch_shapes=[
                *[pltpu.VMEM((tokens, HEAD), F32)] * 2,
                pltpu.VMEM((1, d), F32),
                pltpu.VMEM((tokens, d), BF16),
                pltpu.VMEM((SLOTS, d // WIDE, WIDE, WIDE), BF16),
                pltpu.VMEM((WO_SLOTS, WIDE, d), BF16),
                pltpu.VMEM((nx, 2, tokens, HEAD), BF16),
                pltpu.VMEM((steps, HEAD, 2 * tokens), BF16),
                pltpu.VMEM((chips, 2, tokens, HEAD), BF16),
                pltpu.VMEM((steps, HEAD, 2 * tokens), BF16),
                pltpu.VMEM((steps, 2, 2, own, HEAD), BF16),
                pltpu.VMEM((n // 2, 2, own, HEAD), BF16),
                pltpu.VMEM((own, d), F32),
                *[pltpu.VMEM((2 * tokens, 2 * tokens), F32)] * 2,
                *[pltpu.VMEM((2 * tokens, 2 * tokens), BF16)] * 2,
                *[pltpu.VMEM((1, 2 * tokens), F32)] * 5,
                pltpu.VMEM((HEAD + 16, 2 * tokens), F32),
                pltpu.VMEM((own, d), BF16),
                dma((SLOTS,)), dma((WO_SLOTS,)), dma(()), dma((3,)), dma((nx - 1,)), dma((nx - 1,)), dma((nx, 2)), dma((chips,)), dma((nx, 2)), dma((nx,)), dma((nx,)),
                dma((steps,)), dma((steps,)), dma((steps, 2)), dma((n // 2,)),
            ],
            compiler_params=pltpu.CompilerParams(collective_id=0, has_side_effects=True, vmem_limit_bytes=67043328),
        )(x, gain, turn, cut(wq), cut(wk), cut(wv), wo)

    tokens, whole = P(("dp", "sp"), None), P(None, None)
    return jax.shard_map(
        step,
        mesh=mesh,
        in_specs=(tokens, P(None), whole, whole, whole, whole),
        out_specs=tokens,
        check_vma=False,
    )
```
